32 devices in a mesh: rows: 4 (over y, core), vecs: 8 (over z, x).
Axes of the slice: x: 2, y: 2, z: 4, core: 2. Of those that a mesh axis runs over, the one named last changes fastest.
Arguments:
- vectors: float32 [2048, 2048], P('rows', 'vecs'), may hold values from -6 to 6
- reflectors: float32 [4, 8, 512, 256], P(None, 'rows', 'vecs'), may hold values from -0.4 to 1, as said below
Outputs:
- transformed: float32 [2048, 2048], P('rows', 'vecs')
The draws below stay inside these ranges and needn't reach their ends.
Inputs may be any that keep to these rules, and one draw needn't show every extreme that they name: reflectors[t, b] is unit lower trapezoidal: entry (i, j) is 1 where i == j and 0 where i < j.
All inputs are finite; a program needn't handle non-finite values.
Results may differ from the reference program's by a relative error of at most 0.00026.
Values sent between devices are 32-bit elements; how exact they have to be, the bound alone decides.
No kernel may reach another device: no remote copies, remote signals or barrier semaphores. Data moves between devices by JAX's collectives and lax.ppermute only.
A program may use at most 128 MiB of HBM per device.

```python
import jax
import jax.numpy as jnp
import numpy as np
from jax import lax

SPREAD = 256
SEGMENTS = 4
BLOCKS_DEV = 2
BLOCKS = 8
ROW_COUNT = 2048
VEC_COUNT = 2048
N_ROWS = 4


def draw_reflectors(key, part):
    shape = (SEGMENTS, BLOCKS, 2 * SPREAD, SPREAD)
    row_index = lax.broadcasted_iota(jnp.int32, (2 * SPREAD, SPREAD), 0)
    col_index = lax.broadcasted_iota(jnp.int32, (2 * SPREAD, SPREAD), 1)
    raw = jnp.clip(0.06 * jax.random.normal(jax.random.fold_in(key, 13), shape, jnp.float32), -0.4, 0.4)
    lower_part = jnp.where(row_index == col_index, 1.0, 0.0).astype(jnp.float32)
    return jnp.where(row_index > col_index, raw, lower_part).astype(jnp.float32)


def block_levels(stream_key, dims, shards, low, high):
    level, own = 1.0, jax.random.fold_in(stream_key, 6)
    for axis_at, blocks in shards:
        draws = jnp.exp(jax.random.uniform(jax.random.fold_in(own, axis_at), (blocks,), jnp.float32, low / len(shards), high / len(shards)))
        level = level * jnp.repeat(draws, dims[axis_at] // blocks).reshape([-1 if axis == axis_at else 1 for axis in range(len(dims))])
    return level


def gaussian(stream_key, extent, spread, limit, shards=(), kind=jnp.bfloat16):
    values = spread * jax.random.normal(stream_key, extent, jnp.float32)
    if shards:
        values = values * block_levels(stream_key, extent, shards, -0.22, 0.18)
    return jnp.clip(values, -limit, limit).astype(kind)


def setup_inputs(seed: int = 0) -> dict:
    keys = jax.random.split(jax.random.key(seed), 3)
    vectors = gaussian(keys[0], (ROW_COUNT, VEC_COUNT), 1.0, 6.0, ((0, 4), (1, 8)), jnp.float32)
    reflectors = draw_reflectors(jax.random.fold_in(keys[2], 71), 0)
    return {"vectors": vectors, "reflectors": reflectors}


def invert_upper(matrix):
    size = matrix.shape[-1]
    if size == 1:
        return 1.0 / matrix
    half = size // 2
    upper_left = matrix[:, :half, :half]
    corner = matrix[:, :half, half:]
    lower_right = matrix[:, half:, half:]
    if half * 2 == size:
        count = matrix.shape[0]
        both = invert_upper(jnp.concatenate([upper_left, lower_right], axis=0))
        left_inverse = both[:count]
        right_inverse = both[count:]
    else:
        left_inverse = invert_upper(upper_left)
        right_inverse = invert_upper(lower_right)
    middle = jnp.einsum("bij,bjk->bik", corner, right_inverse, precision=lax.Precision.HIGHEST)
    middle = -jnp.einsum("bij,bjk->bik", left_inverse, middle, precision=lax.Precision.HIGHEST)
    zeros_block = jnp.zeros((matrix.shape[0], size - half, half), matrix.dtype)
    top = jnp.concatenate([left_inverse, middle], axis=2)
    bottom = jnp.concatenate([zeros_block, right_inverse], axis=2)
    return jnp.concatenate([top, bottom], axis=1)


def make_factor(gram):
    return jnp.triu(gram, 1) + 0.5 * jnp.diag(jnp.diagonal(gram))


def reflect(window_rows, vblock, inverse):
    products = jnp.dot(vblock.T, window_rows, precision=lax.Precision.HIGHEST)
    solved = jnp.dot(inverse, products, precision=lax.Precision.HIGHEST)
    return window_rows - jnp.dot(vblock, solved, precision=lax.Precision.HIGHEST)


def reference(vectors, reflectors):
    ordering = []
    for sweep in range(SEGMENTS + N_ROWS - 1):
        for block in range(BLOCKS):
            moment = sweep - (N_ROWS - 1) + block // BLOCKS_DEV
            if 0 <= moment < SEGMENTS:
                ordering.append((moment, block))
    table = jnp.asarray(np.array(ordering, dtype=np.int32))
    padded = jnp.concatenate([vectors, jnp.zeros((SPREAD, vectors.shape[1]), vectors.dtype)], axis=0)

    def advance(index, current):
        moment = table[index, 0]
        block = table[index, 1]
        vblock = reflectors[moment, block]
        start = (block * SPREAD).astype(jnp.int32)
        window_rows = lax.dynamic_slice_in_dim(current, start, 2 * SPREAD, 0)
        gram = jnp.dot(vblock.T, vblock, precision=lax.Precision.HIGHEST)
        inverse = invert_upper(make_factor(gram)[None])[0]
        updated = reflect(window_rows, vblock, inverse)
        return lax.dynamic_update_slice_in_dim(current, updated, start, 0)

    result = lax.fori_loop(0, len(ordering), advance, padded)
    return result[:ROW_COUNT]
```

```python
import functools

import jax
import jax.numpy as jnp
from jax import lax
from jax.experimental import pallas as pl
from jax.experimental.pallas import tpu as pltpu
from jax.sharding import PartitionSpec as P

BASE = 16
BF = jnp.bfloat16
F32 = jnp.float32


def split(value):
    high = value.astype(BF)
    return high, (value - high.astype(F32)).astype(BF)


def dot3(left, right, dims=((1,), (0,))):
    (lh, ll), (rh, rl) = left, right
    run = functools.partial(lax.dot_general, dimension_numbers=(dims, ((), ())), preferred_element_type=F32)
    return run(lh, rh) + (run(lh, rl) + run(ll, rh))


def invert_factor(gram):
    size = gram.shape[0]
    count = size // BASE
    row = lax.broadcasted_iota(jnp.int32, (size, size), 0)
    col = lax.broadcasted_iota(jnp.int32, (size, size), 1)
    factor = jnp.where(row < col, gram, jnp.where(row == col, 0.5 * gram, 0.0))
    same = (row // BASE) == (col // BASE)
    blocks = jnp.where(same, factor, 0.0)
    compact = jnp.sum(blocks.reshape(count, BASE, size), axis=0)
    lane = lax.broadcasted_iota(jnp.int32, (BASE, size), 1) % BASE
    sub = lax.broadcasted_iota(jnp.int32, (BASE, size), 0)
    ones = same.astype(BF)
    stacked = jnp.concatenate([jnp.where(lane == k, compact, 0.0) for k in range(BASE)], axis=0)
    high, low = split(stacked)
    rest = (stacked - high.astype(F32) - low.astype(F32)).astype(BF)
    run = functools.partial(jnp.dot, preferred_element_type=F32)
    spread = run(high, ones) + (run(low, ones) + run(rest, ones))
    small = jnp.where(sub == lane, 1.0, 0.0).astype(F32)
    for k in reversed(range(BASE)):
        column = spread[BASE * k : BASE * (k + 1)]
        pivot = small[k : k + 1] / column[k : k + 1]
        small = jnp.where(sub == k, pivot, small - jnp.where(sub < k, column, 0.0) * pivot)
    inverse = jnp.where(same, jnp.concatenate([small] * count, axis=0), 0.0)
    width = BASE
    while width < size:
        corner = jnp.where(((row // width) % 2 == 0) & ((col // width) == (row // width) + 1), factor, 0.0)
        parts = split(inverse)
        middle = dot3(split(corner), parts)
        inverse = inverse - dot3(parts, split(middle))
        width *= 2
    return inverse


def prepare_kernel(place_ref, *refs, groups):
    chunks = refs[: groups + 1]
    vh_ref, vl_ref, wh_ref, wl_ref, shared_ref, full_ref = refs[groups + 1 :]
    rows = chunks[0].shape[1]
    place = place_ref[0]
    block_count = full_ref.shape[0]
    for k in range(groups):
        line = lax.rem(place // 2 - k + groups, groups) * 2
        own = pl.multiple_of((line + place % 2) * rows, rows)
        other = pl.multiple_of((line + 1 - place % 2) * rows, rows)
        full_ref[:, pl.ds(own, rows), :] = chunks[k][...]
        full_ref[:, pl.ds(other, rows), :] = chunks[groups][k]
    width = full_ref.shape[2]
    parts = []
    for b in range(block_count):
        high, low = split(full_ref[b])
        vh_ref[b] = high
        vl_ref[b] = low
        parts.append((high, low))
    grams = [dot3(v, v, ((0,), (0,))) for v in parts]
    inverses = [invert_factor(g) for g in grams]
    for b in range(block_count):
        weights = dot3(split(inverses[b]), parts[b], ((1,), (1,)))
        wparts = split(weights)
        wh_ref[b] = wparts[0]
        wl_ref[b] = wparts[1]
        if b == block_count - 1:
            bottom = (parts[b][0][width:], parts[b][1][width:])
            shared_ref[...] = dot3(bottom, wparts)


def prepare(place, zs, xs):
    groups = len(zs)
    block_count, rows, width = zs[0].shape
    total = rows * groups * 2
    vm = pl.BlockSpec(memory_space=pltpu.VMEM)
    flops = block_count * 3 * 2 * (total * width * width * 2 + 10 * width**3)
    return pl.pallas_call(
        functools.partial(prepare_kernel, groups=groups),
        in_specs=[pl.BlockSpec(memory_space=pltpu.SMEM)] + [vm] * (groups + 1),
        out_specs=[vm] * 5,
        out_shape=[
            jax.ShapeDtypeStruct((block_count, total, width), BF),
            jax.ShapeDtypeStruct((block_count, total, width), BF),
            jax.ShapeDtypeStruct((block_count, width, total), BF),
            jax.ShapeDtypeStruct((block_count, width, total), BF),
            jax.ShapeDtypeStruct((width, total), F32),
        ],
        scratch_shapes=[pltpu.VMEM((block_count, total, width), F32)],
        cost_estimate=pl.CostEstimate(flops=flops, bytes_accessed=8 * block_count * total * width, transcendentals=0),
        name="prepare",
    )(place, *zs, xs)


def first_kernel(vh, vl, wh, wl, upper, lower, out_upper, out_lower):
    width = upper.shape[0]
    rows = jnp.concatenate([upper[...], lower[...]], axis=0)
    solved = dot3((wh[0], wl[0]), split(rows))
    change = dot3((vh[0], vl[0]), split(solved))
    out_upper[...] = upper[...] - change[:width]
    out_lower[...] = lower[...] - change[width:]


def first(made, upper, lower):
    vm = pl.BlockSpec(memory_space=pltpu.VMEM)
    vh, vl, wh, wl, _ = made
    out = jax.ShapeDtypeStruct(upper.shape, F32)
    return pl.pallas_call(
        first_kernel,
        in_specs=[vm] * 6,
        out_specs=[vm] * 2,
        out_shape=[out, out],
        cost_estimate=pl.CostEstimate(flops=6 * vh.shape[1] * vh.shape[2] * upper.shape[1] * 2, bytes_accessed=0, transcendentals=0),
        name="first",
    )(vh, vl, wh, wl, upper, lower)


def second_kernel(vh, vl, wh, wl, shared, sent, lower, above, beneath, out_shared, out_lower):
    last = vh.shape[0] - 1
    width = lower.shape[0]
    rows = jnp.concatenate([lower[...], beneath[...]], axis=0)
    solved = dot3((wh[last], wl[last]), split(rows))
    change = dot3((vh[last, :width], vl[last, :width]), split(solved))
    out_lower[...] = lower[...] - change
    both = jnp.concatenate([above[...], sent[...]], axis=0)
    out_shared[...] = sent[...] - dot3(split(shared[...]), split(both))


def second(made, shared, sent, lower, above, beneath):
    vm = pl.BlockSpec(memory_space=pltpu.VMEM)
    vh, vl, wh, wl, _ = made
    out = jax.ShapeDtypeStruct(lower.shape, F32)
    return pl.pallas_call(
        second_kernel,
        in_specs=[vm] * 9,
        out_specs=[vm] * 2,
        out_shape=[out, out],
        cost_estimate=pl.CostEstimate(flops=6 * vh.shape[1] * vh.shape[2] * lower.shape[1] * 2, bytes_accessed=0, transcendentals=0),
        name="second",
    )(vh, vl, wh, wl, shared, sent, lower, above, beneath)


def gathered(piece):
    count = lax.axis_size("vecs")
    groups = count // 2
    zs = [piece]
    for k in range(1, groups):
        pairs = [(d, ((d // 2 + k) % groups) * 2 + d % 2) for d in range(count)]
        zs.append(lax.ppermute(piece, "vecs", pairs))
    xs = lax.ppermute(jnp.stack(zs), "vecs", [(d, d ^ 1) for d in range(count)])
    return zs, xs


def local(vectors, reflectors):
    width = reflectors.shape[3]
    assert reflectors.shape[1] == 2 and vectors.shape[0] == 2 * width
    sections = lax.axis_size("rows")
    topmost = lax.axis_index("rows") == 0
    place = lax.axis_index("vecs").astype(jnp.int32)[None]
    up = [(r, (r - 1) % sections) for r in range(sections)]
    down = [(r, (r + 1) % sections) for r in range(sections)]
    upper, lower = vectors[:width], vectors[width:]
    tail = jnp.zeros_like(upper)
    pieces = [gathered(reflectors[t]) for t in range(reflectors.shape[0])]
    made = [prepare(place, *p) for p in pieces]
    for t in range(len(made)):
        shared = lax.ppermute(made[t][4], "rows", down)
        upper, lower = first(made[t], upper, lower)
        sent = jnp.where(topmost, tail, upper)
        beneath = lax.ppermute(sent, "rows", up)
        above = lax.ppermute(lower, "rows", down)
        updated, lower = second(made[t], shared, sent, lower, above, beneath)
        tail = updated
        upper = jnp.where(topmost, upper, updated)
    return jnp.concatenate([upper, lower], axis=0)


def solution(mesh):
    placed = (P("rows", "vecs"), P(None, "rows", "vecs", None))
    return jax.shard_map(
        local, mesh=mesh, in_specs=placed, out_specs=P("rows", "vecs"), check_vma=False
    )
```
